32 devices in a mesh: row: 4 (over y, x), col: 8 (over z, core).
Axes of the slice: x: 2, y: 2, z: 4, core: 2. Of those that a mesh axis runs over, the one named last changes fastest.
Arguments:
- tokens: bfloat16 [4096, 2048], P(('row', 'col')), may hold values from -6 to 6
- expert_ids: int32 [4096, 8], P(('row', 'col')), may hold values from 0 to 31, all different within a row; in each aligned block of 128 rows (0 to 127, 128 to 255, ...) at most 40 rows name the same one
- gate_probs: float32 [4096, 8], P(('row', 'col')), may hold values from 0.05 to 0.5
- w_gate: bfloat16 [32, 2048, 768], P(('row', 'col')), may hold values from -0.125 to 0.125
- w_up: bfloat16 [32, 2048, 768], P(('row', 'col')), may hold values from -0.125 to 0.125
- w_down: bfloat16 [32, 768, 2048], P(('row', 'col')), may hold values from -0.21875 to 0.21875
Outputs:
- mixed: bfloat16 [4096, 2048], P(('row', 'col'))
The draws below stay inside these ranges and needn't reach their ends.
Inputs may be any that keep to these rules, and one draw needn't show every extreme that they name: `expert_ids`: each row names 8 different experts; among the rows of one device (aligned blocks of 128 rows) no expert is named more than 40 times.
All inputs are finite; a program needn't handle non-finite values.
Results may differ from the reference program's by a relative error of at most 0.0058.
Values may be sent and summed in bfloat16 or wider, within the bound.
A program may use at most 128 MiB of HBM per device.

```python
import math
import jax
import jax.numpy as jnp
import numpy as np
from jax import lax

D = 2048
FF = 768
TOPK = 8
TOK_DEV = 128
EXPERTS = 32
TOKENS = 4096
SLOTS = 40
N_ROW = 4
N_COL = 8


def level_of(stream_key, extent, shards, smallest, high):
    def one(axis_at, blocks):
        draws = jax.random.uniform(jax.random.fold_in(jax.random.fold_in(stream_key, 6), axis_at), (blocks,), jnp.float32, smallest / len(shards), high / len(shards))
        return jnp.repeat(jnp.exp(draws), extent[axis_at] // blocks).reshape((-1,) + (1,) * (len(extent) - axis_at - 1))

    loudness = one(*shards[0])
    for cut in shards[1:]:
        loudness = loudness * one(*cut)
    return loudness


def shared_out(own_key, own, number, rows, count, top, most, slope):
    order = jax.random.permutation(own_key, count)
    crowded, ordinary = load_shares(count, rows * top, most, slope, True), load_shares(count, rows * top, most, slope, False)
    places = jnp.arange(count)

    def named(lengths, rotation):
        used = int((lengths > 0).sum())
        fixed = max(1, used // 4)
        shifted = fixed + (places - fixed + rotation * (used - fixed)) % max(1, count - fixed)
        return jnp.zeros((count,), jnp.int32).at[order[jnp.where(places < fixed, places, shifted)]].set(jnp.asarray(lengths, jnp.int32))

    lengths = jnp.where(number % 4 == 0, named(crowded, number // 4), named(ordinary, number - number // 4 - 1))
    mixed = jax.random.permutation(jax.random.fold_in(own, 3), count)
    source_of, taker = mixed[0:count // 2 * 2:2], mixed[1:count // 2 * 2:2]
    room = jnp.minimum(lengths[source_of] - 1, most - lengths[taker]) // 2
    room = jnp.where((source_of == order[0]) | (taker == order[0]) | (lengths[taker] == 0), 0, jnp.maximum(room, 0))
    shifted = jax.random.randint(jax.random.fold_in(own, 4), (count // 2,), 0, 1 << 20) % (room + 1)
    lengths = lengths.at[source_of].add(-shifted).at[taker].add(shifted)
    members = jnp.searchsorted(jnp.cumsum(lengths), jnp.arange(rows * top), side="right").astype(jnp.int32)
    listing = members.reshape(top, rows).T
    listing = listing[jax.random.permutation(jax.random.fold_in(own, 1), rows)]
    rotation = jax.random.randint(jax.random.fold_in(own, 2), (rows, 1), 0, top)
    return jnp.take_along_axis(listing, (jnp.arange(top)[None, :] + rotation) % top, axis=1)


def load_shares(number_of, total, most, slope, full):
    loads = [(1 << 20) // math.isqrt(rank ** slope) + 1 for rank in range(1, number_of + 1)]
    largest = most if full else min(most, max(-(-total // number_of), total * loads[0] // sum(loads)))
    least = 1 if total - largest >= number_of - 1 else 0
    counts, rest = [largest] + [least] * (number_of - 1), total - largest - least * (number_of - 1)
    while rest > 0:
        movable = [i for i in range(1, number_of) if counts[i] < largest] or [i for i in range(1, number_of) if counts[i] < most]
        whole, left = sum([loads[i] for i in movable]), rest
        for i in movable:
            addition = min(most - counts[i], max(1, left * loads[i] // whole), rest)
            counts[i] = counts[i] + addition
            rest = rest - addition
    return np.array(counts)


def gaussian(key, shape, deviation, bound, cuts=(), held_as=jnp.bfloat16):
    drawn = deviation * jax.random.normal(key, shape, jnp.float32)
    if cuts:
        drawn = drawn * level_of(key, shape, cuts, -0.22, 0.18)
    return jnp.clip(drawn, -bound, bound).astype(held_as)


def setup_inputs(seed: int = 0) -> dict:
    seeds = jax.random.split(jax.random.key(seed), 7)
    tokens = gaussian(seeds[0], (TOKENS, D), 1.0, 6.0, ((0, 32),))
    expert_ids_keys = jax.random.split(jax.random.fold_in(seeds[1], 1), TOKENS // TOK_DEV)
    expert_ids_turns = jax.random.permutation(jax.random.fold_in(seeds[1], 3), TOKENS // TOK_DEV)
    expert_ids = jax.vmap(lambda own, number: shared_out(jax.random.fold_in(seeds[1], 2), own, number, TOK_DEV, EXPERTS, TOPK, SLOTS, 2))(expert_ids_keys, expert_ids_turns).reshape((TOKENS, TOPK))
    gate_probs = jnp.clip(0.05 + 0.45 * jax.random.uniform(seeds[2], (TOKENS, TOPK), jnp.float32) ** level_of(seeds[2], (TOKENS, TOPK), ((0, 32),), -0.2, 0.2), 0.05, 0.5)
    w_gate = gaussian(seeds[3], (EXPERTS, D, FF), D ** -0.5, 0.125, ((0, 32),))
    w_up = gaussian(seeds[4], (EXPERTS, D, FF), D ** -0.5, 0.125, ((0, 32),))
    w_down = gaussian(seeds[5], (EXPERTS, FF, D), FF ** -0.5, 0.21875, ((0, 32),))
    return dict(tokens=tokens, expert_ids=expert_ids, gate_probs=gate_probs, w_gate=w_gate, w_up=w_up, w_down=w_down)


def reference(tokens, expert_ids, gate_probs, w_gate, w_up, w_down):
    sources = N_ROW * N_COL
    flat_ids = expert_ids.reshape(sources, TOK_DEV * TOPK)
    onehot = (flat_ids[:, :, None] == jnp.arange(EXPERTS, dtype=jnp.int32)[None, None, :]).astype(jnp.int32)
    rank = jnp.sum((jnp.cumsum(onehot, axis=1) - 1) * onehot, axis=2).astype(jnp.int32)
    source = jnp.arange(sources, dtype=jnp.int32)[:, None]
    position = (flat_ids * (sources * SLOTS) + source * SLOTS + rank).reshape(-1).astype(jnp.int32)
    token_of = (jnp.arange(TOKENS * TOPK, dtype=jnp.int32) // TOPK).astype(jnp.int32)
    owner = jnp.full((EXPERTS * sources * SLOTS,), -1, jnp.int32).at[position].set(token_of)
    owner = owner.reshape(EXPERTS, sources * SLOTS)

    def one_expert(index):
        picks = owner[index]
        rows = tokens[jnp.maximum(picks, 0)]
        rows = jnp.where((picks >= 0)[:, None], rows, jnp.zeros((), tokens.dtype))
        gate = jnp.dot(rows, w_gate[index], preferred_element_type=jnp.float32)
        up = jnp.dot(rows, w_up[index], preferred_element_type=jnp.float32)
        hidden = (jax.nn.silu(gate) * up).astype(jnp.bfloat16)
        return jnp.dot(hidden, w_down[index], preferred_element_type=jnp.float32).astype(jnp.bfloat16)

    outputs = lax.map(one_expert, jnp.arange(EXPERTS, dtype=jnp.int32))
    picked = outputs.reshape(-1, D)[position].reshape(TOKENS, TOPK, D).astype(jnp.float32)
    mixed = jnp.sum(gate_probs.astype(jnp.float32)[:, :, None] * picked, axis=1)
    return mixed.astype(jnp.bfloat16)
```

```python
import functools
import math

import jax
import jax.numpy as jnp
from jax import lax
from jax.experimental import pallas as pl
from jax.experimental.pallas import tpu as pltpu
from jax.sharding import PartitionSpec as P

MESH = pl.DeviceIdType.MESH
BF16 = jnp.bfloat16
F32 = jnp.float32


def moe_kernel(
    rows, cols, slots, group,
    meta_in, tok_in, wg_in, wu_in, wd_in, out_ref,
    meta, tok, wg, wu, wd, disp, comb, hid, xs, xr, yr, pr, acc, zs, zr,
    load_sem, meta_send, meta_recv, ztok_send, ztok_recv, ctok_send, ctok_recv,
    x_send, x_recv, y_send, y_recv, p_send, p_recv, z_send, z_recv,
):
    r = lax.axis_index("row")
    c = lax.axis_index("col")
    chips = cols // 2
    chip, core = c // 2, c % 2
    mate = 2 * chip + (1 - core)
    count, width = tok_in.shape
    per = group // 2
    chunks = chips // per
    part = group * slots
    total = rows * part
    hidden = wg.shape[1]
    f_tile = math.gcd(hidden, 256)
    d_tile = math.gcd(width, 512)

    def remote(src, dst, send, recv, row, col):
        return pltpu.make_async_remote_copy(
            src_ref=src, dst_ref=dst, send_sem=send, recv_sem=recv,
            device_id=(row, col), device_id_type=MESH,
        )

    load_tok = pltpu.make_async_copy(tok_in, tok.at[0, 0], load_sem.at[0])
    load_meta = pltpu.make_async_copy(meta_in, meta.at[0], load_sem.at[1])
    load_w = [
        pltpu.make_async_copy(wg_in.at[0], wg, load_sem.at[2]),
        pltpu.make_async_copy(wu_in.at[0], wu, load_sem.at[3]),
        pltpu.make_async_copy(wd_in.at[0], wd, load_sem.at[4]),
    ]
    load_tok.start()
    load_meta.start()

    barrier = pltpu.get_barrier_semaphore()
    for d in range(1, cols):
        pl.semaphore_signal(barrier, inc=1, device_id=(r, (c + d) % cols), device_id_type=MESH)
    for j in range(1, rows):
        pl.semaphore_signal(barrier, inc=1, device_id=((r + j) % rows, c), device_id_type=MESH)
    pl.semaphore_wait(barrier, cols - 1 + rows - 1)

    load_tok.wait()
    tok_out = remote(tok.at[0, 0], tok.at[0, 1], ctok_send.at[0], ctok_recv.at[0], r, mate)
    tok_out.start()
    load_meta.wait()
    meta_out = []
    for d in range(1, cols):
        far, other = d // 2, d % 2
        target = 2 * ((chip + chips - far) % chips) + (core if other == 0 else 1 - core)
        copy = remote(meta.at[0], meta.at[d], meta_send.at[d], meta_recv.at[d], r, target)
        copy.start()
        meta_out.append(copy)
    ztok = [None]
    for d in range(1, chips):
        target = 2 * ((chip + chips - d) % chips) + core
        copy = remote(tok.at[0, 0], tok.at[d, 0], ztok_send.at[d], ztok_recv.at[d], r, target)
        copy.start()
        ztok.append(copy)
    for copy in load_w:
        copy.start()
    ctok = [tok_out] + [
        remote(tok.at[d, 0], tok.at[d, 1], ctok_send.at[d], ctok_recv.at[d], r, mate)
        for d in range(1, chips)
    ]
    for copy in meta_out:
        copy.wait()

    earlier = (
        lax.broadcasted_iota(jnp.int32, (count, count), 0)
        < lax.broadcasted_iota(jnp.int32, (count, count), 1)
    ).astype(BF16)
    slot_of = lax.broadcasted_iota(jnp.int32, (part, count), 0).astype(F32)
    lane_rows = 16
    row_id = lax.broadcasted_iota(jnp.int32, (lane_rows, count), 0)
    choices = meta_in.shape[0] // 2

    def route(i):
        for s in range(group):
            m = meta[i * group + s]
            ids, probs = m[:choices], m[choices:]
            named = jnp.zeros((lane_rows, count), F32)
            weights = []
            for j in range(rows):
                expert = (((r + j) % rows) * cols + c).astype(F32)
                hit = (ids == expert).astype(F32)
                named = jnp.where(row_id == j, jnp.sum(hit, axis=0, keepdims=True), named)
                weights.append(jnp.sum(hit * probs, axis=0, keepdims=True))
            rank = jnp.dot(named.astype(BF16), earlier, preferred_element_type=F32)
            key = jnp.where(named > 0.5, rank + float(s * slots), -1.0)
            for j in range(rows):
                one = (slot_of == key[j:j + 1, :]).astype(F32)
                disp[j * part:(j + 1) * part, s * count:(s + 1) * count] = one.astype(BF16)
                comb[i, j * part:(j + 1) * part, s * count:(s + 1) * count] = (
                    one * weights[j]
                ).astype(BF16)

    x_out, y_out, p_out, z_out = {}, {}, {}, {}

    def dispatch(i):
        for d in range(i * per, (i + 1) * per):
            if d > 0:
                ztok[d].wait_recv()
                ctok[d].start()
        route(i)
        for d in range(i * per, (i + 1) * per):
            ctok[d].wait_recv()

        def tile(n, _):
            at = pl.ds(pl.multiple_of(n * d_tile, d_tile), d_tile)
            block = tok[i * per:(i + 1) * per, :, :, at].reshape(group * count, d_tile)
            res = jnp.dot(disp[...], block, preferred_element_type=F32).astype(BF16)
            xr[i, 0, :, at] = res[:part]
            xs[i, :, :, at] = res[part:].reshape(rows - 1, part, d_tile)
            return 0

        lax.fori_loop(0, width // d_tile, tile, 0)
        for j in range(1, rows):
            copy = remote(
                xs.at[i, j - 1], xr.at[i, j], x_send.at[i, j], x_recv.at[i, j],
                (r + j) % rows, c,
            )
            copy.start()
            x_out[i, j] = copy

    def experts(i, first):
        for j in range(1, rows):
            x_out[i, j].wait()
        if first:
            for copy in load_w:
                copy.wait()

        def up_tile(n, _):
            at = pl.ds(pl.multiple_of(n * f_tile, f_tile), f_tile)
            x = xr[i].reshape(total, width)
            gate = jnp.dot(x, wg[:, at], preferred_element_type=F32)
            up = jnp.dot(x, wu[:, at], preferred_element_type=F32)
            hid[:, at] = (gate / (1.0 + jnp.exp(-gate)) * up).astype(BF16)
            return 0

        lax.fori_loop(0, hidden // f_tile, up_tile, 0)

        def down_tile(n, _):
            at = pl.ds(pl.multiple_of(n * d_tile, d_tile), d_tile)
            res = jnp.dot(hid[...], wd[:, at], preferred_element_type=F32).astype(BF16)
            yr[i, 0, :, at] = res[:part]
            xs[i, :, :, at] = res[part:].reshape(rows - 1, part, d_tile)
            return 0

        lax.fori_loop(0, width // d_tile, down_tile, 0)
        for j in range(1, rows):
            copy = remote(
                xs.at[i, j - 1], yr.at[i, j], y_send.at[i, j], y_recv.at[i, j],
                (r + rows - j) % rows, c,
            )
            copy.start()
            y_out[i, j] = copy

    def combine(i):
        for j in range(1, rows):
            y_out[i, j].wait()

        def tile(n, _):
            at = pl.ds(pl.multiple_of(n * d_tile, d_tile), d_tile)
            y = yr[i, :, :, at].reshape(total, d_tile)
            res = lax.dot_general(
                comb[i], y, (((0,), (0,)), ((), ())), preferred_element_type=F32
            )
            for p in range(per):
                d = i * per + p
                acc[d, :, at] = res[2 * p * count:(2 * p + 1) * count]
                tok[d, 1, :, at] = res[(2 * p + 1) * count:(2 * p + 2) * count].astype(BF16)
            return 0

        lax.fori_loop(0, width // d_tile, tile, 0)
        for d in range(i * per, (i + 1) * per):
            copy = remote(tok.at[d, 1], pr.at[d], p_send.at[d], p_recv.at[d], r, mate)
            copy.start()
            p_out[d] = copy

    def reduce_cores(i):
        for d in range(i * per, (i + 1) * per):
            p_out[d].wait()
            if d == 0:
                continue
            zs[d - 1] = (acc[d] + pr[d].astype(F32)).astype(BF16)
            copy = remote(
                zs.at[d - 1], zr.at[chips - d - 1], z_send.at[d], z_recv.at[chips - d],
                r, 2 * ((chip + d) % chips) + core,
            )
            copy.start()
            z_out[d] = copy

    order = list(range(1, chunks)) + [0]
    dispatch(0)
    for i in range(1, chunks):
        dispatch(i)
        if i > 1:
            experts(order[i - 2], i == 2)
    for n in range(max(chunks - 2, 0), chunks):
        experts(order[n], n == 0)
    for n in range(chunks):
        combine(order[n])
        if n > 0:
            reduce_cores(order[n - 1])
    reduce_cores(order[-1])
    for d in range(1, chips):
        z_out[d].wait()
    for d in range(1, chips):
        ztok[d].wait_send()
    for d in range(chips):
        ctok[d].wait_send()
    result = acc[0] + pr[0].astype(F32)
    for d in range(1, chips):
        result = result + zr[d - 1].astype(F32)
    out_ref[...] = result.astype(BF16)


def body(tokens, expert_ids, gate_probs, w_gate, w_up, w_down):
    count, choices = expert_ids.shape
    width = tokens.shape[1]
    hidden = w_gate.shape[2]
    rows = lax.axis_size("row")
    cols = lax.axis_size("col")
    slots = 5 * count * choices // (4 * rows * cols * w_gate.shape[0])
    group = 2
    while group * slots % 16:
        group *= 2
    chips = cols // 2
    chunks = cols // group
    part = group * slots
    meta = jnp.concatenate([expert_ids.astype(F32).T, gate_probs.T], axis=0)
    any_spec = pl.BlockSpec(memory_space=pl.ANY)
    dma = pltpu.SemaphoreType.DMA
    scratch = [
        pltpu.VMEM((cols, 2 * choices, count), F32),
        pltpu.VMEM((chips, 2, count, width), BF16),
        pltpu.VMEM((width, hidden), BF16),
        pltpu.VMEM((width, hidden), BF16),
        pltpu.VMEM((hidden, width), BF16),
        pltpu.VMEM((rows * part, group * count), BF16),
        pltpu.VMEM((chunks, rows * part, group * count), BF16),
        pltpu.VMEM((rows * part, hidden), BF16),
        pltpu.VMEM((chunks, rows - 1, part, width), BF16),
        pltpu.VMEM((chunks, rows, part, width), BF16),
        pltpu.VMEM((chunks, rows, part, width), BF16),
        pltpu.VMEM((chips, count, width), BF16),
        pltpu.VMEM((chips, count, width), F32),
        pltpu.VMEM((chips - 1, count, width), BF16),
        pltpu.VMEM((chips - 1, count, width), BF16),
        dma((5,)),
        dma((cols,)), dma((cols,)),
        dma((chips,)), dma((chips,)),
        dma((chips,)), dma((chips,)),
        dma((chunks, rows)), dma((chunks, rows)),
        dma((chunks, rows)), dma((chunks, rows)),
        dma((chips,)), dma((chips,)),
        dma((chips,)), dma((chips,)),
    ]
    return pl.pallas_call(
        functools.partial(moe_kernel, rows, cols, slots, group),
        out_shape=jax.ShapeDtypeStruct((count, width), BF16),
        in_specs=[any_spec] * 5,
        out_specs=pl.BlockSpec(memory_space=pltpu.VMEM),
        scratch_shapes=scratch,
        compiler_params=pltpu.CompilerParams(
            collective_id=0, has_side_effects=True, vmem_limit_bytes=67043328
        ),
    )(meta, tokens, w_gate, w_up, w_down)


def solution(mesh):
    in_specs = (
        P(("row", "col"), None),
        P(("row", "col"), None),
        P(("row", "col"), None),
        P(("row", "col"), None, None),
        P(("row", "col"), None, None),
        P(("row", "col"), None, None),
    )
    out_specs = P(("row", "col"), None)
    return jax.shard_map(body, mesh=mesh, in_specs=in_specs, out_specs=out_specs, check_vma=False)
```

```python
import functools
import math

import jax
import jax.numpy as jnp
from jax import lax
from jax.experimental import pallas as pl
from jax.experimental.pallas import tpu as pltpu
from jax.sharding import PartitionSpec as P

MESH = pl.DeviceIdType.MESH
BF16 = jnp.bfloat16
F32 = jnp.float32


def moe_kernel(
    rows, cols, slots, group,
    meta_in, tok_in, wg_in, wu_in, wd_in, out_ref,
    meta, tok, wg, wu, wd, disp, comb, hid, xs, xr, yr, pr, acc, zs, zr,
    load_sem, meta_send, meta_recv, ztok_send, ztok_recv, ctok_send, ctok_recv,
    x_send, x_recv, y_send, y_recv, p_send, p_recv, z_send, z_recv,
):
    r = lax.axis_index("row")
    c = lax.axis_index("col")
    chips = cols // 2
    chip, core = c // 2, c % 2
    mate = 2 * chip + (1 - core)
    count, width = tok_in.shape
    per = group // 2
    chunks = chips // per
    part = group * slots
    total = rows * part
    hidden = wg.shape[1]
    f_tile = math.gcd(hidden, 256)
    d_tile = math.gcd(width, 512)

    def remote(src, dst, send, recv, row, col):
        return pltpu.make_async_remote_copy(
            src_ref=src, dst_ref=dst, send_sem=send, recv_sem=recv,
            device_id=(row, col), device_id_type=MESH,
        )

    short = jnp.minimum(chip, chips - 1 - chip)
    side = jnp.where(2 * chip < chips, 1, -1)
    order, signs = [chip], [None]
    for p in range(1, chips):
        both = p <= 2 * short
        sign = jnp.where(both, 1 if p % 2 else -1, side)
        far = jnp.where(both, (p + 1) // 2, p - short)
        order.append(chip + sign * far)
        signs.append(sign)

    load_tok = pltpu.make_async_copy(tok_in, tok.at[chip, 0], load_sem.at[0])
    load_meta = pltpu.make_async_copy(meta_in, meta.at[chip, 0], load_sem.at[1])
    load_w = [
        pltpu.make_async_copy(wg_in.at[0], wg, load_sem.at[2]),
        pltpu.make_async_copy(wu_in.at[0], wu, load_sem.at[3]),
        pltpu.make_async_copy(wd_in.at[0], wd, load_sem.at[4]),
    ]
    load_tok.start()
    load_meta.start()

    barrier = pltpu.get_barrier_semaphore()
    for d in range(1, cols):
        pl.semaphore_signal(barrier, inc=1, device_id=(r, (c + d) % cols), device_id_type=MESH)
    for j in range(1, rows):
        pl.semaphore_signal(barrier, inc=1, device_id=((r + j) % rows, c), device_id_type=MESH)
    pl.semaphore_wait(barrier, cols - 1 + rows - 1)

    def hop(q, send, to):
        return remote(
            tok.at[q, 0], tok.at[q, 0], ztok_send.at[send], ztok_recv.at[q],
            r, 2 * ((to + chips) % chips) + core,
        )

    def onward(p, act):
        if p == 0:
            @pl.when(chip > 0)
            def _():
                act(hop(chip, 0, chip - 1))

            @pl.when(chip < chips - 1)
            def _():
                act(hop(chip, chips, chip + 1))
        else:
            to = chip - signs[p]

            @pl.when((to >= 0) & (to < chips))
            def _():
                act(hop(order[p], p, to))

    ctok = [
        remote(tok.at[q, 0], tok.at[q, 1], ctok_send.at[p], ctok_recv.at[p], r, mate)
        for p, q in enumerate(order)
    ]
    load_tok.wait()
    ctok[0].start()
    load_meta.wait()

    def meta_copy(d, t, slot):
        far, other = d // 2, d % 2
        return remote(
            meta.at[chip, 0], meta.at[slot, other], meta_send.at[d], meta_recv.at[slot, other],
            r, 2 * t + (core if other == 0 else 1 - core),
        )

    for d in range(1, cols):
        meta_copy(d, (chip + d // 2) % chips, chip).start()
    onward(0, lambda copy: copy.start())
    for copy in load_w:
        copy.start()
    for d in range(1, cols):
        t = (chip + d // 2) % chips
        meta_copy(d, t, t).wait()

    earlier = (
        lax.broadcasted_iota(jnp.int32, (count, count), 0)
        < lax.broadcasted_iota(jnp.int32, (count, count), 1)
    ).astype(BF16)
    slot_of = lax.broadcasted_iota(jnp.int32, (part, count), 0).astype(F32)
    lane_rows = 16
    row_id = lax.broadcasted_iota(jnp.int32, (lane_rows, count), 0)
    choices = meta_in.shape[0] // 2

    def route(i):
        for s in range(group):
            m = meta[order[i * per + s // 2], s % 2]
            ids, probs = m[:choices], m[choices:]
            named = jnp.zeros((lane_rows, count), F32)
            weights = []
            for j in range(rows):
                expert = (((r + j) % rows) * cols + c).astype(F32)
                hit = (ids == expert).astype(F32)
                named = jnp.where(row_id == j, jnp.sum(hit, axis=0, keepdims=True), named)
                weights.append(jnp.sum(hit * probs, axis=0, keepdims=True))
            rank = jnp.dot(named.astype(BF16), earlier, preferred_element_type=F32)
            key = jnp.where(named > 0.5, rank + float(s * slots), -1.0)
            for j in range(rows):
                one = (slot_of == key[j:j + 1, :]).astype(F32)
                disp[j * part:(j + 1) * part, s * count:(s + 1) * count] = one.astype(BF16)
                comb[i, j * part:(j + 1) * part, s * count:(s + 1) * count] = (
                    one * weights[j]
                ).astype(BF16)

    x_out, y_out, p_out, z_out = {}, {}, {}, {}

    def dispatch(i):
        for d in range(i * per, (i + 1) * per):
            if d > 0:
                hop(order[d], d, chip).wait_recv()
                onward(d, lambda copy: copy.start())
                ctok[d].start()
        route(i)
        for d in range(i * per, (i + 1) * per):
            ctok[d].wait_recv()

        def tile(n, _):
            at = pl.ds(pl.multiple_of(n * d_tile, d_tile), d_tile)
            block = jnp.concatenate(
                [tok[q, :, :, at].reshape(2 * count, d_tile) for q in order[i * per:(i + 1) * per]]
            )
            res = jnp.dot(disp[...], block, preferred_element_type=F32).astype(BF16)
            xr[i, 0, :, at] = res[:part]
            xs[i, :, :, at] = res[part:].reshape(rows - 1, part, d_tile)
            return 0

        lax.fori_loop(0, width // d_tile, tile, 0)
        for j in range(1, rows):
            copy = remote(
                xs.at[i, j - 1], xr.at[i, j], x_send.at[i, j], x_recv.at[i, j],
                (r + j) % rows, c,
            )
            copy.start()
            x_out[i, j] = copy

    def experts(i, first):
        for j in range(1, rows):
            x_out[i, j].wait()
        if first:
            for copy in load_w:
                copy.wait()

        def up_tile(n, _):
            at = pl.ds(pl.multiple_of(n * f_tile, f_tile), f_tile)
            x = xr[i].reshape(total, width)
            gate = jnp.dot(x, wg[:, at], preferred_element_type=F32)
            up = jnp.dot(x, wu[:, at], preferred_element_type=F32)
            hid[:, at] = (gate / (1.0 + jnp.exp(-gate)) * up).astype(BF16)
            return 0

        lax.fori_loop(0, hidden // f_tile, up_tile, 0)

        def down_tile(n, _):
            at = pl.ds(pl.multiple_of(n * d_tile, d_tile), d_tile)
            res = jnp.dot(hid[...], wd[:, at], preferred_element_type=F32).astype(BF16)
            yr[i, 0, :, at] = res[:part]
            xs[i, :, :, at] = res[part:].reshape(rows - 1, part, d_tile)
            return 0

        lax.fori_loop(0, width // d_tile, down_tile, 0)
        for j in range(1, rows):
            copy = remote(
                xs.at[i, j - 1], yr.at[i, j], y_send.at[i, j], y_recv.at[i, j],
                (r + rows - j) % rows, c,
            )
            copy.start()
            y_out[i, j] = copy

    def combine(i):
        for j in range(1, rows):
            y_out[i, j].wait()

        def tile(n, _):
            at = pl.ds(pl.multiple_of(n * d_tile, d_tile), d_tile)
            y = yr[i, :, :, at].reshape(total, d_tile)
            res = lax.dot_general(
                comb[i], y, (((0,), (0,)), ((), ())), preferred_element_type=F32
            )
            for p in range(per):
                d = i * per + p
                acc[d, :, at] = res[2 * p * count:(2 * p + 1) * count]
                tok[order[d], 1, :, at] = res[(2 * p + 1) * count:(2 * p + 2) * count].astype(BF16)
            return 0

        lax.fori_loop(0, width // d_tile, tile, 0)
        for d in range(i * per, (i + 1) * per):
            copy = remote(tok.at[order[d], 1], pr.at[d], p_send.at[d], p_recv.at[d], r, mate)
            copy.start()
            p_out[d] = copy

    def reduce_cores(i):
        for d in range(i * per, (i + 1) * per):
            p_out[d].wait()
            if d == 0:
                continue
            zs[d - 1] = (acc[d] + pr[d].astype(F32)).astype(BF16)
            copy = remote(
                zs.at[d - 1], zr.at[chip], z_send.at[d], z_recv.at[chip], r, 2 * order[d] + core
            )
            copy.start()
            z_out[d] = copy

    turn = list(range(1, chunks)) + [0]
    dispatch(0)
    for i in range(1, chunks):
        dispatch(i)
        if i > 1:
            experts(turn[i - 2], i == 2)
    for n in range(max(chunks - 2, 0), chunks):
        experts(turn[n], n == 0)
    for n in range(chunks):
        combine(turn[n])
        reduce_cores(turn[n])
    result = acc[0] + pr[0].astype(F32)
    for d in range(1, chips):
        q = order[d]
        z_out[d].wait_send()
        remote(zs.at[d - 1], zr.at[q], z_send.at[d], z_recv.at[q], r, 2 * q + core).wait_recv()
        result = result + zr[q].astype(F32)
    for d in range(chips):
        onward(d, lambda copy: copy.wait_send())
        ctok[d].wait_send()
    out_ref[...] = result.astype(BF16)


def body(tokens, expert_ids, gate_probs, w_gate, w_up, w_down):
    count, choices = expert_ids.shape
    width = tokens.shape[1]
    hidden = w_gate.shape[2]
    rows = lax.axis_size("row")
    cols = lax.axis_size("col")
    slots = 5 * count * choices // (4 * rows * cols * w_gate.shape[0])
    group = 2
    while group * slots % 16:
        group *= 2
    chips = cols // 2
    chunks = cols // group
    part = group * slots
    meta = jnp.concatenate([expert_ids.astype(F32).T, gate_probs.T], axis=0)
    any_spec = pl.BlockSpec(memory_space=pl.ANY)
    dma = pltpu.SemaphoreType.DMA
    scratch = [
        pltpu.VMEM((chips, 2, 2 * choices, count), F32),
        pltpu.VMEM((chips, 2, count, width), BF16),
        pltpu.VMEM((width, hidden), BF16),
        pltpu.VMEM((width, hidden), BF16),
        pltpu.VMEM((hidden, width), BF16),
        pltpu.VMEM((rows * part, group * count), BF16),
        pltpu.VMEM((chunks, rows * part, group * count), BF16),
        pltpu.VMEM((rows * part, hidden), BF16),
        pltpu.VMEM((chunks, rows - 1, part, width), BF16),
        pltpu.VMEM((chunks, rows, part, width), BF16),
        pltpu.VMEM((chunks, rows, part, width), BF16),
        pltpu.VMEM((chips, count, width), BF16),
        pltpu.VMEM((chips, count, width), F32),
        pltpu.VMEM((chips - 1, count, width), BF16),
        pltpu.VMEM((chips, count, width), BF16),
        dma((5,)),
        dma((cols,)), dma((chips, 2)),
        dma((chips + 1,)), dma((chips,)),
        dma((chips,)), dma((chips,)),
        dma((chunks, rows)), dma((chunks, rows)),
        dma((chunks, rows)), dma((chunks, rows)),
        dma((chips,)), dma((chips,)),
        dma((chips,)), dma((chips,)),
    ]
    return pl.pallas_call(
        functools.partial(moe_kernel, rows, cols, slots, group),
        out_shape=jax.ShapeDtypeStruct((count, width), BF16),
        in_specs=[any_spec] * 5,
        out_specs=pl.BlockSpec(memory_space=pltpu.VMEM),
        scratch_shapes=scratch,
        compiler_params=pltpu.CompilerParams(
            collective_id=0, has_side_effects=True, vmem_limit_bytes=67043328
        ),
    )(meta, tokens, w_gate, w_up, w_down)


def solution(mesh):
    in_specs = (
        P(("row", "col"), None),
        P(("row", "col"), None),
        P(("row", "col"), None),
        P(("row", "col"), None, None),
        P(("row", "col"), None, None),
        P(("row", "col"), None, None),
    )
    out_specs = P(("row", "col"), None)
    return jax.shard_map(body, mesh=mesh, in_specs=in_specs, out_specs=out_specs, check_vma=False)
```

```python
import functools
import math

import jax
import jax.numpy as jnp
from jax import lax
from jax.experimental import pallas as pl
from jax.experimental.pallas import tpu as pltpu
from jax.sharding import PartitionSpec as P

MESH = pl.DeviceIdType.MESH
BF16 = jnp.bfloat16
F32 = jnp.float32
PIECES = 2


def moe_kernel(
    rows, cols, slots, group, pieces,
    ids_in, probs_in, tok_in, wg_in, wu_in, wd_in, out_ref,
    ids_all, probs_all, tok, wg, wu, wd, disp, comb, hid, xs, xr, yr, pr, acc, zs, zr,
    load_sem, ids_send, ids_recv, probs_send, probs_recv, ztok_send, ztok_recv, ctok_send, ctok_recv,
    x_send, x_recv, y_send, y_recv, p_send, p_recv, z_send, z_recv,
):
    r = lax.axis_index("row")
    c = lax.axis_index("col")
    chips = cols // 2
    chip, core = c // 2, c % 2
    mate = 2 * chip + (1 - core)
    count, width = tok_in.shape
    per = group // 2
    chunks = chips // per
    part = group * slots
    total = rows * part
    hidden = wg.shape[1]
    f_tile = math.gcd(hidden, 256)
    d_tile = math.gcd(width // pieces, 512)
    piece = width // pieces

    def remote(src, dst, send, recv, row, col):
        return pltpu.make_async_remote_copy(
            src_ref=src, dst_ref=dst, send_sem=send, recv_sem=recv,
            device_id=(row, col), device_id_type=MESH,
        )

    short = jnp.minimum(chip, chips - 1 - chip)
    side = jnp.where(2 * chip < chips, 1, -1)
    order, signs = [chip], [None]
    for p in range(1, chips):
        both = p <= 2 * short
        sign = jnp.where(both, 1 if p % 2 else -1, side)
        far = jnp.where(both, (p + 1) // 2, p - short)
        order.append(chip + sign * far)
        signs.append(sign)

    load_tok = pltpu.make_async_copy(tok_in, tok.at[chip, 0], load_sem.at[0])
    load_ids = pltpu.make_async_copy(ids_in, ids_all.at[chip, 0], load_sem.at[1])
    load_probs = pltpu.make_async_copy(probs_in, probs_all.at[chip, 0], load_sem.at[5])
    load_w = [
        pltpu.make_async_copy(wg_in.at[0], wg, load_sem.at[2]),
        pltpu.make_async_copy(wu_in.at[0], wu, load_sem.at[3]),
        pltpu.make_async_copy(wd_in.at[0], wd, load_sem.at[4]),
    ]
    load_tok.start()
    load_ids.start()
    load_probs.start()

    barrier = pltpu.get_barrier_semaphore()
    for d in range(1, cols):
        pl.semaphore_signal(barrier, inc=1, device_id=(r, (c + d) % cols), device_id_type=MESH)
    for j in range(1, rows):
        pl.semaphore_signal(barrier, inc=1, device_id=((r + j) % rows, c), device_id_type=MESH)
    pl.semaphore_wait(barrier, cols - 1 + rows - 1)

    def hop(q, send, to):
        return remote(
            tok.at[q, 0], tok.at[q, 0], ztok_send.at[send], ztok_recv.at[q],
            r, 2 * ((to + chips) % chips) + core,
        )

    def onward(p, act):
        if p == 0:
            @pl.when(chip > 0)
            def _():
                act(hop(chip, 0, chip - 1))

            @pl.when(chip < chips - 1)
            def _():
                act(hop(chip, chips, chip + 1))
        else:
            to = chip - signs[p]

            @pl.when((to >= 0) & (to < chips))
            def _():
                act(hop(order[p], p, to))

    ctok = [
        remote(tok.at[q, 0], tok.at[q, 1], ctok_send.at[p], ctok_recv.at[p], r, mate)
        for p, q in enumerate(order)
    ]
    load_tok.wait()
    ctok[0].start()
    load_ids.wait()
    load_probs.wait()

    def routing(d, t, slot):
        far, other = d // 2, d % 2
        to = 2 * t + (core if other == 0 else 1 - core)
        return (
            remote(
                ids_all.at[chip, 0], ids_all.at[slot, other],
                ids_send.at[d], ids_recv.at[slot, other], r, to,
            ),
            remote(
                probs_all.at[chip, 0], probs_all.at[slot, other],
                probs_send.at[d], probs_recv.at[slot, other], r, to,
            ),
        )

    for d in range(1, cols):
        for copy in routing(d, (chip + d // 2) % chips, chip):
            copy.start()
    onward(0, lambda copy: copy.start())
    for copy in load_w:
        copy.start()
    for d in range(1, cols):
        t = (chip + d // 2) % chips
        for copy in routing(d, t, t):
            copy.wait()

    earlier = (
        lax.broadcasted_iota(jnp.int32, (count, count), 0)
        < lax.broadcasted_iota(jnp.int32, (count, count), 1)
    ).astype(BF16)
    slot_of = lax.broadcasted_iota(jnp.int32, (part, count), 0).astype(F32)
    lane_rows = 16
    row_id = lax.broadcasted_iota(jnp.int32, (lane_rows, count), 0)

    def route(i):
        for s in range(group):
            ids = ids_all[order[i * per + s // 2], s % 2]
            probs = probs_all[order[i * per + s // 2], s % 2]
            named = jnp.zeros((lane_rows, count), F32)
            weights = []
            for j in range(rows):
                expert = ((r + j) % rows) * cols + c
                hit = (ids == expert).astype(F32)
                named = jnp.where(row_id == j, jnp.sum(hit, axis=0, keepdims=True), named)
                weights.append(jnp.sum(hit * probs, axis=0, keepdims=True))
            rank = jnp.dot(named.astype(BF16), earlier, preferred_element_type=F32)
            key = jnp.where(named > 0.5, rank + float(s * slots), -1.0)
            for j in range(rows):
                one = (slot_of == key[j:j + 1, :]).astype(F32)
                disp[j * part:(j + 1) * part, s * count:(s + 1) * count] = one.astype(BF16)
                comb[i, j * part:(j + 1) * part, s * count:(s + 1) * count] = (
                    one * weights[j]
                ).astype(BF16)

    x_out, y_out, p_out, z_out = {}, {}, {}, {}

    def dispatch(i):
        for d in range(i * per, (i + 1) * per):
            if d > 0:
                hop(order[d], d, chip).wait_recv()
                onward(d, lambda copy: copy.start())
                ctok[d].start()
        route(i)
        for d in range(i * per, (i + 1) * per):
            ctok[d].wait_recv()

        def tile(n, _):
            at = pl.ds(pl.multiple_of(n * d_tile, d_tile), d_tile)
            block = jnp.concatenate(
                [tok[q, :, :, at].reshape(2 * count, d_tile) for q in order[i * per:(i + 1) * per]]
            )
            res = jnp.dot(disp[...], block, preferred_element_type=F32).astype(BF16)
            xr[i, 0, :, at] = res[:part]
            xs[i, :, :, at] = res[part:].reshape(rows - 1, part, d_tile)
            return 0

        lax.fori_loop(0, width // d_tile, tile, 0)
        for j in range(1, rows):
            copy = remote(
                xs.at[i, j - 1], xr.at[i, j], x_send.at[i, j], x_recv.at[i, j],
                (r + j) % rows, c,
            )
            copy.start()
            x_out[i, j] = copy

    def experts(i, first):
        for j in range(1, rows):
            x_out[i, j].wait()
        if first:
            for copy in load_w:
                copy.wait()

        def up_tile(n, _):
            at = pl.ds(pl.multiple_of(n * f_tile, f_tile), f_tile)
            x = xr[i].reshape(total, width)
            gate = jnp.dot(x, wg[:, at], preferred_element_type=F32)
            up = jnp.dot(x, wu[:, at], preferred_element_type=F32)
            hid[:, at] = (gate / (1.0 + jnp.exp(-gate)) * up).astype(BF16)
            return 0

        lax.fori_loop(0, hidden // f_tile, up_tile, 0)

        def down_tile(n, _):
            at = pl.ds(pl.multiple_of(n * d_tile, d_tile), d_tile)
            res = jnp.dot(hid[...], wd[:, at], preferred_element_type=F32).astype(BF16)
            yr[i, 0, :, at] = res[:part]
            xs[i, :, :, at] = res[part:].reshape(rows - 1, part, d_tile)
            return 0

        for h in range(pieces):
            at = pl.ds(h * piece, piece)
            lax.fori_loop(h * piece // d_tile, (h + 1) * piece // d_tile, down_tile, 0)
            for j in range(1, rows):
                copy = remote(
                    xs.at[i, j - 1, :, at], yr.at[i, j, :, at],
                    y_send.at[i, j, h], y_recv.at[i, j, h], (r + rows - j) % rows, c,
                )
                copy.start()
                y_out[i, j, h] = copy

    def combine(i, h):
        for j in range(1, rows):
            y_out[i, j, h].wait()

        def tile(n, _):
            at = pl.ds(pl.multiple_of(n * d_tile, d_tile), d_tile)
            y = yr[i, :, :, at].reshape(total, d_tile)
            res = lax.dot_general(
                comb[i], y, (((0,), (0,)), ((), ())), preferred_element_type=F32
            )
            for p in range(per):
                d = i * per + p
                acc[d, :, at] = res[2 * p * count:(2 * p + 1) * count]
                tok[order[d], 1, :, at] = res[(2 * p + 1) * count:(2 * p + 2) * count].astype(BF16)
            return 0

        lax.fori_loop(h * piece // d_tile, (h + 1) * piece // d_tile, tile, 0)
        at = pl.ds(h * piece, piece)
        for d in range(i * per, (i + 1) * per):
            copy = remote(
                tok.at[order[d], 1, :, at], pr.at[d, :, at], p_send.at[d, h], p_recv.at[d, h],
                r, mate,
            )
            copy.start()
            p_out[d, h] = copy

    def partial_copy(d, h, slot):
        at = pl.ds(h * piece, piece)
        return remote(
            zs.at[d - 1, :, at], zr.at[slot, :, at], z_send.at[d, h], z_recv.at[slot, h],
            r, 2 * order[d] + core,
        )

    def reduce_cores(i, h):
        at = pl.ds(h * piece, piece)
        for d in range(i * per, (i + 1) * per):
            p_out[d, h].wait()
            if d > 0:
                zs[d - 1, :, at] = (acc[d, :, at] + pr[d, :, at].astype(F32)).astype(BF16)
                partial_copy(d, h, chip).start()

    turn = list(range(chunks // 2, chunks)) + list(range(chunks // 2 - 1, -1, -1))
    for i in range(chunks):
        dispatch(i)
    for n in range(chunks):
        experts(turn[n], n == 0)
    for n in range(chunks):
        for h in range(pieces):
            combine(turn[n], h)
            reduce_cores(turn[n], h)
    for h in range(pieces):
        at = pl.ds(h * piece, piece)
        result = acc[0, :, at] + pr[0, :, at].astype(F32)
        for d in range(1, chips):
            partial_copy(d, h, order[d]).wait()
            result = result + zr[order[d], :, at].astype(F32)
        out_ref[:, at] = result.astype(BF16)
    for d in range(chips):
        onward(d, lambda copy: copy.wait_send())
        ctok[d].wait_send()


def body(tokens, expert_ids, gate_probs, w_gate, w_up, w_down):
    count, choices = expert_ids.shape
    width = tokens.shape[1]
    hidden = w_gate.shape[2]
    rows = lax.axis_size("row")
    cols = lax.axis_size("col")
    slots = 5 * count * choices // (4 * rows * cols * w_gate.shape[0])
    group = 2
    while group * slots % 16:
        group *= 2
    chips = cols // 2
    chunks = cols // group
    part = group * slots
    any_spec = pl.BlockSpec(memory_space=pl.ANY)
    dma = pltpu.SemaphoreType.DMA
    scratch = [
        pltpu.VMEM((chips, 2, choices, count), jnp.int32),
        pltpu.VMEM((chips, 2, choices, count), F32),
        pltpu.VMEM((chips, 2, count, width), BF16),
        pltpu.VMEM((width, hidden), BF16),
        pltpu.VMEM((width, hidden), BF16),
        pltpu.VMEM((hidden, width), BF16),
        pltpu.VMEM((rows * part, group * count), BF16),
        pltpu.VMEM((chunks, rows * part, group * count), BF16),
        pltpu.VMEM((rows * part, hidden), BF16),
        pltpu.VMEM((chunks, rows - 1, part, width), BF16),
        pltpu.VMEM((chunks, rows, part, width), BF16),
        pltpu.VMEM((chunks, rows, part, width), BF16),
        pltpu.VMEM((chips, count, width), BF16),
        pltpu.VMEM((chips, count, width), F32),
        pltpu.VMEM((chips - 1, count, width), BF16),
        pltpu.VMEM((chips, count, width), BF16),
        dma((6,)),
        dma((cols,)), dma((chips, 2)),
        dma((cols,)), dma((chips, 2)),
        dma((chips + 1,)), dma((chips,)),
        dma((chips,)), dma((chips,)),
        dma((chunks, rows)), dma((chunks, rows)),
        dma((chunks, rows, PIECES)), dma((chunks, rows, PIECES)),
        dma((chips, PIECES)), dma((chips, PIECES)),
        dma((chips, PIECES)), dma((chips, PIECES)),
    ]
    return pl.pallas_call(
        functools.partial(moe_kernel, rows, cols, slots, group, PIECES),
        out_shape=jax.ShapeDtypeStruct((count, width), BF16),
        in_specs=[any_spec] * 6,
        out_specs=pl.BlockSpec(memory_space=pltpu.VMEM),
        scratch_shapes=scratch,
        compiler_params=pltpu.CompilerParams(
            collective_id=0, has_side_effects=True, vmem_limit_bytes=67043328
        ),
    )(expert_ids.T, gate_probs.T, tokens, w_gate, w_up, w_down)


def solution(mesh):
    in_specs = (
        P(("row", "col"), None),
        P(("row", "col"), None),
        P(("row", "col"), None),
        P(("row", "col"), None, None),
        P(("row", "col"), None, None),
        P(("row", "col"), None, None),
    )
    out_specs = P(("row", "col"), None)
    return jax.shard_map(body, mesh=mesh, in_specs=in_specs, out_specs=out_specs, check_vma=False)
```

```python
import functools
import math

import jax
import jax.numpy as jnp
from jax import lax
from jax.experimental import pallas as pl
from jax.experimental.pallas import tpu as pltpu
from jax.sharding import PartitionSpec as P

MESH = pl.DeviceIdType.MESH
BF16 = jnp.bfloat16
F32 = jnp.float32
PIECES = 2


def moe_kernel(
    rows, cols, slots, group, pieces,
    ids_in, probs_in, tok_in, wg_in, wu_in, wd_in, out_ref,
    ids_all, probs_all, tok, wg, wu, wd, disp, comb, hid, xs, xr, yr, pr, acc, zs, zr,
    load_sem, ids_send, ids_recv, probs_send, probs_recv, ztok_send, ztok_recv, ctok_send, ctok_recv,
    x_send, x_recv, y_send, y_recv, p_send, p_recv, z_send, z_recv,
):
    r = lax.axis_index("row")
    c = lax.axis_index("col")
    chips = cols // 2
    chip, core = c // 2, c % 2
    mate = 2 * chip + (1 - core)
    count, width = tok_in.shape
    per = group // 2
    chunks = chips // per
    part = group * slots
    total = rows * part
    hidden = wg.shape[1]
    f_tile = math.gcd(hidden, 256)
    d_tile = math.gcd(width // pieces, 512)
    piece = width // pieces

    def remote(src, dst, send, recv, row, col):
        return pltpu.make_async_remote_copy(
            src_ref=src, dst_ref=dst, send_sem=send, recv_sem=recv,
            device_id=(row, col), device_id_type=MESH,
        )

    short = jnp.minimum(chip, chips - 1 - chip)
    side = jnp.where(2 * chip < chips, 1, -1)
    order, signs = [chip], [None]
    for p in range(1, chips):
        both = p <= 2 * short
        sign = jnp.where(both, 1 if p % 2 else -1, side)
        far = jnp.where(both, (p + 1) // 2, p - short)
        order.append(chip + sign * far)
        signs.append(sign)

    load_tok = pltpu.make_async_copy(tok_in, tok.at[chip, 0], load_sem.at[0])
    load_ids = pltpu.make_async_copy(ids_in, ids_all.at[chip, 0], load_sem.at[1])
    load_probs = pltpu.make_async_copy(probs_in, probs_all.at[chip, 0], load_sem.at[5])
    load_w = [
        pltpu.make_async_copy(wg_in.at[0], wg, load_sem.at[2]),
        pltpu.make_async_copy(wu_in.at[0], wu, load_sem.at[3]),
        pltpu.make_async_copy(wd_in.at[0], wd, load_sem.at[4]),
    ]
    load_tok.start()
    load_ids.start()
    load_probs.start()

    barrier = pltpu.get_barrier_semaphore()
    for d in range(1, cols):
        pl.semaphore_signal(barrier, inc=1, device_id=(r, (c + d) % cols), device_id_type=MESH)
    for j in range(1, rows):
        pl.semaphore_signal(barrier, inc=1, device_id=((r + j) % rows, c), device_id_type=MESH)
    pl.semaphore_wait(barrier, cols - 1 + rows - 1)

    def hop(q, send, to):
        return remote(
            tok.at[q, 0], tok.at[q, 0], ztok_send.at[send], ztok_recv.at[q],
            r, 2 * ((to + chips) % chips) + core,
        )

    def onward(p, act):
        if p == 0:
            @pl.when(chip > 0)
            def _():
                act(hop(chip, 0, chip - 1))

            @pl.when(chip < chips - 1)
            def _():
                act(hop(chip, chips, chip + 1))
        else:
            to = chip - signs[p]

            @pl.when((to >= 0) & (to < chips))
            def _():
                act(hop(order[p], p, to))

    ctok = [
        remote(tok.at[q, 0], tok.at[q, 1], ctok_send.at[p], ctok_recv.at[p], r, mate)
        for p, q in enumerate(order)
    ]
    load_tok.wait()
    ctok[0].start()
    load_ids.wait()
    load_probs.wait()

    def routing(d, t, slot):
        far, other = d // 2, d % 2
        to = 2 * t + (core if other == 0 else 1 - core)
        return (
            remote(
                ids_all.at[chip, 0], ids_all.at[slot, other],
                ids_send.at[d], ids_recv.at[slot, other], r, to,
            ),
            remote(
                probs_all.at[chip, 0], probs_all.at[slot, other],
                probs_send.at[d], probs_recv.at[slot, other], r, to,
            ),
        )

    for d in range(1, cols):
        for copy in routing(d, (chip + d // 2) % chips, chip):
            copy.start()
    onward(0, lambda copy: copy.start())
    for copy in load_w:
        copy.start()
    earlier = (
        lax.broadcasted_iota(jnp.int32, (count, count), 0)
        < lax.broadcasted_iota(jnp.int32, (count, count), 1)
    ).astype(BF16)
    slot_of = lax.broadcasted_iota(jnp.int32, (part, count), 0).astype(F32)
    lane_rows = 16
    row_id = lax.broadcasted_iota(jnp.int32, (lane_rows, count), 0)

    def route(i):
        for s in range(group):
            ids = ids_all[order[i * per + s // 2], s % 2]
            probs = probs_all[order[i * per + s // 2], s % 2]
            named = jnp.zeros((lane_rows, count), F32)
            weights = []
            for j in range(rows):
                expert = ((r + j) % rows) * cols + c
                hit = (ids == expert).astype(F32)
                named = jnp.where(row_id == j, jnp.sum(hit, axis=0, keepdims=True), named)
                weights.append(jnp.sum(hit * probs, axis=0, keepdims=True))
            rank = jnp.dot(named.astype(BF16), earlier, preferred_element_type=F32)
            key = jnp.where(named > 0.5, rank + float(s * slots), -1.0)
            for j in range(rows):
                one = (slot_of == key[j:j + 1, :]).astype(F32)
                disp[j * part:(j + 1) * part, s * count:(s + 1) * count] = one.astype(BF16)
                comb[i, j * part:(j + 1) * part, s * count:(s + 1) * count] = (
                    one * weights[j]
                ).astype(BF16)

    x_out, y_out, p_out, z_out = {}, {}, {}, {}

    def dispatch(i):
        for d in range(i * per, (i + 1) * per):
            if d > 0:
                hop(order[d], d, chip).wait_recv()
                onward(d, lambda copy: copy.start())
                ctok[d].start()
            for other in range(0 if d > 0 else 1, 2):
                for copy in routing(other, order[d], order[d]):
                    copy.wait_recv()
        route(i)
        for d in range(i * per, (i + 1) * per):
            ctok[d].wait_recv()

        def tile(n, _):
            at = pl.ds(pl.multiple_of(n * d_tile, d_tile), d_tile)
            block = jnp.concatenate(
                [tok[q, :, :, at].reshape(2 * count, d_tile) for q in order[i * per:(i + 1) * per]]
            )
            res = jnp.dot(disp[...], block, preferred_element_type=F32).astype(BF16)
            xr[i, 0, :, at] = res[:part]
            xs[i, :, :, at] = res[part:].reshape(rows - 1, part, d_tile)
            return 0

        lax.fori_loop(0, width // d_tile, tile, 0)
        for j in range(1, rows):
            copy = remote(
                xs.at[i, j - 1], xr.at[i, j], x_send.at[i, j], x_recv.at[i, j],
                (r + j) % rows, c,
            )
            copy.start()
            x_out[i, j] = copy

    def experts(i, first):
        for j in range(1, rows):
            x_out[i, j].wait()
        if first:
            for copy in load_w:
                copy.wait()

        def up_tile(n, _):
            at = pl.ds(pl.multiple_of(n * f_tile, f_tile), f_tile)
            x = xr[i].reshape(total, width)
            gate = jnp.dot(x, wg[:, at], preferred_element_type=F32)
            up = jnp.dot(x, wu[:, at], preferred_element_type=F32)
            hid[:, at] = (gate / (1.0 + jnp.exp(-gate)) * up).astype(BF16)
            return 0

        lax.fori_loop(0, hidden // f_tile, up_tile, 0)

        def down_tile(n, _):
            at = pl.ds(pl.multiple_of(n * d_tile, d_tile), d_tile)
            res = jnp.dot(hid[...], wd[:, at], preferred_element_type=F32).astype(BF16)
            yr[i, 0, :, at] = res[:part]
            xs[i, :, :, at] = res[part:].reshape(rows - 1, part, d_tile)
            return 0

        for h in range(pieces):
            at = pl.ds(h * piece, piece)
            lax.fori_loop(h * piece // d_tile, (h + 1) * piece // d_tile, down_tile, 0)
            for j in range(1, rows):
                copy = remote(
                    xs.at[i, j - 1, :, at], yr.at[i, j, :, at],
                    y_send.at[i, j, h], y_recv.at[i, j, h], (r + rows - j) % rows, c,
                )
                copy.start()
                y_out[i, j, h] = copy

    def combine(i, h):
        for j in range(1, rows):
            y_out[i, j, h].wait()

        def tile(n, _):
            at = pl.ds(pl.multiple_of(n * d_tile, d_tile), d_tile)
            y = yr[i, :, :, at].reshape(total, d_tile)
            res = lax.dot_general(
                comb[i], y, (((0,), (0,)), ((), ())), preferred_element_type=F32
            )
            for p in range(per):
                d = i * per + p
                acc[d, :, at] = res[2 * p * count:(2 * p + 1) * count]
                tok[order[d], 1, :, at] = res[(2 * p + 1) * count:(2 * p + 2) * count].astype(BF16)
            return 0

        lax.fori_loop(h * piece // d_tile, (h + 1) * piece // d_tile, tile, 0)
        at = pl.ds(h * piece, piece)
        for d in range(i * per, (i + 1) * per):
            copy = remote(
                tok.at[order[d], 1, :, at], pr.at[d, :, at], p_send.at[d, h], p_recv.at[d, h],
                r, mate,
            )
            copy.start()
            p_out[d, h] = copy

    def partial_copy(d, h, slot):
        at = pl.ds(h * piece, piece)
        return remote(
            zs.at[d - 1, :, at], zr.at[slot, :, at], z_send.at[d, h], z_recv.at[slot, h],
            r, 2 * order[d] + core,
        )

    def reduce_cores(i, h):
        at = pl.ds(h * piece, piece)
        for d in range(i * per, (i + 1) * per):
            p_out[d, h].wait()
            if d > 0:
                zs[d - 1, :, at] = (acc[d, :, at] + pr[d, :, at].astype(F32)).astype(BF16)
                partial_copy(d, h, chip).start()

    turn = list(range(chunks // 2, chunks)) + list(range(chunks // 2 - 1, -1, -1))
    for i in range(chunks):
        dispatch(i)
    for n in range(chunks):
        experts(turn[n], n == 0)
    for n in range(chunks):
        for h in range(pieces):
            combine(turn[n], h)
            reduce_cores(turn[n], h)
    for h in range(pieces):
        at = pl.ds(h * piece, piece)
        result = acc[0, :, at] + pr[0, :, at].astype(F32)
        for d in range(1, chips):
            partial_copy(d, h, order[d]).wait()
            result = result + zr[order[d], :, at].astype(F32)
        out_ref[:, at] = result.astype(BF16)
    for d in range(1, cols):
        for copy in routing(d, (chip + d // 2) % chips, chip):
            copy.wait_send()
    for d in range(chips):
        onward(d, lambda copy: copy.wait_send())
        ctok[d].wait_send()


def body(tokens, expert_ids, gate_probs, w_gate, w_up, w_down):
    count, choices = expert_ids.shape
    width = tokens.shape[1]
    hidden = w_gate.shape[2]
    rows = lax.axis_size("row")
    cols = lax.axis_size("col")
    slots = 5 * count * choices // (4 * rows * cols * w_gate.shape[0])
    group = 2
    while group * slots % 16:
        group *= 2
    chips = cols // 2
    chunks = cols // group
    part = group * slots
    any_spec = pl.BlockSpec(memory_space=pl.ANY)
    dma = pltpu.SemaphoreType.DMA
    scratch = [
        pltpu.VMEM((chips, 2, choices, count), jnp.int32),
        pltpu.VMEM((chips, 2, choices, count), F32),
        pltpu.VMEM((chips, 2, count, width), BF16),
        pltpu.VMEM((width, hidden), BF16),
        pltpu.VMEM((width, hidden), BF16),
        pltpu.VMEM((hidden, width), BF16),
        pltpu.VMEM((rows * part, group * count), BF16),
        pltpu.VMEM((chunks, rows * part, group * count), BF16),
        pltpu.VMEM((rows * part, hidden), BF16),
        pltpu.VMEM((chunks, rows - 1, part, width), BF16),
        pltpu.VMEM((chunks, rows, part, width), BF16),
        pltpu.VMEM((chunks, rows, part, width), BF16),
        pltpu.VMEM((chips, count, width), BF16),
        pltpu.VMEM((chips, count, width), F32),
        pltpu.VMEM((chips - 1, count, width), BF16),
        pltpu.VMEM((chips, count, width), BF16),
        dma((6,)),
        dma((cols,)), dma((chips, 2)),
        dma((cols,)), dma((chips, 2)),
        dma((chips + 1,)), dma((chips,)),
        dma((chips,)), dma((chips,)),
        dma((chunks, rows)), dma((chunks, rows)),
        dma((chunks, rows, PIECES)), dma((chunks, rows, PIECES)),
        dma((chips, PIECES)), dma((chips, PIECES)),
        dma((chips, PIECES)), dma((chips, PIECES)),
    ]
    return pl.pallas_call(
        functools.partial(moe_kernel, rows, cols, slots, group, PIECES),
        out_shape=jax.ShapeDtypeStruct((count, width), BF16),
        in_specs=[any_spec] * 6,
        out_specs=pl.BlockSpec(memory_space=pltpu.VMEM),
        scratch_shapes=scratch,
        compiler_params=pltpu.CompilerParams(
            collective_id=0, has_side_effects=True, vmem_limit_bytes=67043328
        ),
    )(expert_ids.T, gate_probs.T, tokens, w_gate, w_up, w_down)


def solution(mesh):
    in_specs = (
        P(("row", "col"), None),
        P(("row", "col"), None),
        P(("row", "col"), None),
        P(("row", "col"), None, None),
        P(("row", "col"), None, None),
        P(("row", "col"), None, None),
    )
    out_specs = P(("row", "col"), None)
    return jax.shard_map(body, mesh=mesh, in_specs=in_specs, out_specs=out_specs, check_vma=False)
```
